32 devices in a mesh: dim: 8 (over y, x, core), batch: 4 (over z).
Axes of the slice: x: 2, y: 2, z: 4, core: 2. Of those that a mesh axis runs over, the one named last changes fastest.
Arguments:
- start: float32 [1024, 4096], P('batch', 'dim'), may hold values from -6 to 6
- increments: float32 [3, 1024, 4096], P(None, 'batch', 'dim'), may hold values from -0.75 to 0.75
- w_in: bfloat16 [4096, 4096], P(None, 'dim'), may hold values from -0.09375 to 0.09375
- w_out: bfloat16 [4096, 4096], P('dim'), may hold values from -0.09375 to 0.09375
- initial: float32 [], replicated, may hold values from 4 to 5.5
Outputs:
- residual: float32 [1024], P('batch')
- grad_in: float32 [4096, 4096], P('batch', 'dim')
- grad_out: float32 [4096, 4096], P('dim', 'batch')
The draws below stay inside these ranges and needn't reach their ends.
All inputs are finite; a program needn't handle non-finite values.
Results may differ from the reference program's by a relative error of at most 0.0051.
Values may be sent and summed in bfloat16 or wider, within the bound.
No kernel may reach another device: no remote copies, remote signals or barrier semaphores. Data moves between devices by JAX's collectives and lax.ppermute only.
A program may use at most 128 MiB of HBM per device.

```python
import math
import jax
import jax.numpy as jnp
from jax import lax

D = 4096
H = 4096
STEPS = 3
PATHS = 1024


def block_levels(stream_key, shape, cuts, low, top_value):
    def one(axis_at, blocks):
        steps = jax.random.uniform(jax.random.fold_in(jax.random.fold_in(stream_key, 6), axis_at), (blocks,), jnp.float32, low / len(cuts), top_value / len(cuts))
        return jnp.repeat(jnp.exp(steps), shape[axis_at] // blocks).reshape((-1,) + (1,) * (len(shape) - axis_at - 1))

    loudness = one(*cuts[0])
    for cut in cuts[1:]:
        loudness = loudness * one(*cut)
    return loudness


def noise(rng, extent, deviation, bound, cuts=(), kind=jnp.bfloat16):
    values = jax.random.normal(rng, extent, jnp.float32) * deviation
    if len(cuts) > 0:
        values = block_levels(rng, extent, cuts, -0.22, 0.18) * values
    return jnp.clip(values, min=-bound, max=bound).astype(kind)


def setup_inputs(seed: int = 0) -> dict:
    key_of = jax.random.split(jax.random.key(seed), 6)
    return {
        "start": noise(key_of[0], (PATHS, D), 1.0, 6.0, ((0, 4), (1, 8)), jnp.float32),
        "increments": noise(key_of[1], (STEPS, PATHS, D), 0.125, 0.75, ((1, 4), (2, 8)), jnp.float32),
        "w_in": noise(key_of[2], (D, H), D ** -0.5, 0.09375, ((1, 8),)),
        "w_out": noise(key_of[3], (H, D), H ** -0.5, 0.09375, ((0, 8),)),
        "initial": jnp.clip(jax.random.uniform(key_of[4], (), jnp.float32, 4.0, 5.5), 4.0, 5.5),
    }


time_step = 1.0 / 64.0
lam_coef = 50.0
noise_coef = math.sqrt(2.0)

def reference(start, increments, w_in, w_out, initial):
    zscale = 2.0 / math.sqrt(D)
    state = start
    saved = []
    ysum = jnp.zeros((start.shape[0],), jnp.float32)
    for step in range(STEPS):
        inc = increments[step]
        xb = state.astype(jnp.bfloat16)
        hidden = jnp.dot(xb, w_in, preferred_element_type=jnp.float32)
        act = jax.nn.silu(hidden).astype(jnp.bfloat16)
        zval = zscale * jnp.dot(act, w_out, preferred_element_type=jnp.float32)
        ysum = ysum + 0.5 * lam_coef * time_step * lax.optimization_barrier(jnp.sum(zval * zval, 1)) + lax.optimization_barrier(jnp.sum(zval * inc, 1))
        saved.append((xb, hidden, act, zval))
        state = state + noise_coef * inc
    norm_sq = lax.optimization_barrier(jnp.sum(state * state, 1))
    residual = initial + ysum - jnp.log((1.0 + norm_sq) * 0.5)
    grad_in = jnp.zeros(w_in.shape, jnp.float32)
    grad_out = jnp.zeros(w_out.shape, jnp.float32)
    for step in range(STEPS):
        xb, hidden, act, zval = saved[step]
        gz = (zscale * residual[:, None] * (lam_coef * time_step * zval + increments[step])).astype(jnp.bfloat16)
        grad_out = grad_out + jnp.dot(act.T, gz, preferred_element_type=jnp.float32)
        ga = jnp.dot(gz, w_out.T, preferred_element_type=jnp.float32)
        sig = jax.nn.sigmoid(hidden)
        gh = (ga * sig * (1.0 + hidden * (1.0 - sig))).astype(jnp.bfloat16)
        grad_in = grad_in + jnp.dot(xb.T, gh, preferred_element_type=jnp.float32)
    return (residual, grad_in, grad_out)
```

```python
import functools
import math

import jax
import jax.numpy as jnp
from jax import lax
from jax.sharding import PartitionSpec as P

time_step = 1.0 / 64.0
lam_coef = 50.0
noise_coef = math.sqrt(2.0)
bf16 = jnp.bfloat16
f32 = jnp.float32


def swap(v, axis, size, mask):
    return lax.ppermute(v, axis, [(i, i ^ mask) for i in range(size)])


def mm(a, b, ca=1, cb=0):
    return lax.dot_general(a, b, (((ca,), (cb,)), ((), ())), preferred_element_type=f32)


def gather_cols(v, nd, flip):
    width = v.shape[1]
    bits = [1 << k for k in range(1, nd.bit_length() - 1)]
    if flip:
        bits = bits[::-1]
    pieces = {0: v}
    for bit in bits:
        masks = sorted(pieces)
        sent = pieces[0] if len(masks) == 1 else jnp.concatenate([pieces[m] for m in masks], 1)
        got = swap(sent, "dim", nd, bit)
        for i, m in enumerate(masks):
            pieces[m ^ bit] = got[:, i * width : (i + 1) * width]
    near = jnp.concatenate([pieces[m] for m in sorted(pieces)], 1)
    return near, swap(near, "dim", nd, 1)


def scatter_sum(near, far, nd, width, flip):
    near = near + swap(far, "dim", nd, 1).astype(f32)
    half = nd // 2
    pieces = {2 * i: near[:, i * width : (i + 1) * width] for i in range(half)}
    bits = [1 << k for k in range(1, nd.bit_length() - 1)]
    if flip:
        bits = bits[::-1]
    for bit in bits:
        away = sorted(m for m in pieces if m & bit)
        sent = jnp.concatenate([pieces[m].astype(bf16) for m in away], 1)
        got = swap(sent, "dim", nd, bit)
        for i, m in enumerate(away):
            pieces[m ^ bit] = pieces[m ^ bit] + got[:, i * width : (i + 1) * width].astype(f32)
            del pieces[m]
    return pieces[0]


def gather_batch(v, nb):
    if nb == 4:
        near = swap(v, "batch", nb, 1)
        two = jnp.concatenate([v, near], 0)
        mid = lax.ppermute(two, "batch", [(1, 2), (2, 1)])
        end = lax.ppermute(mid, "batch", [(1, 0), (2, 3)])
        return jnp.concatenate([two, mid + end], 0)
    bit = 1
    while bit < nb:
        v = jnp.concatenate([v, swap(v, "batch", nb, bit)], 0)
        bit *= 2
    return v


def column_share(near, far, nd, nb, width, scale=None):
    d = lax.axis_index("dim")
    b = lax.axis_index("batch")
    span = nd * width // nb
    share = span // nd

    def of(dest):
        start = dest * span + d * share
        mask = (start // width) ^ d
        at = (mask >> 1) * width + start % width
        one = lax.dynamic_slice_in_dim(near, at, share, 1)
        two = lax.dynamic_slice_in_dim(far, at, share, 1)
        out = jnp.where((mask & 1) == 1, two, one)
        if scale is not None:
            out = (out.astype(f32) * scale).astype(bf16)
        return out

    got = [of(b)] + [swap(of(b ^ j), "batch", nb, j) for j in range(1, nb)]
    if nb == 4:
        inner = (b == 1) | (b == 2)
        got[2], got[3] = jnp.where(inner, got[3], got[2]), jnp.where(inner, got[2], got[3])
    return got


def on_device(nd, nb, chunks, start, increments, w_in, w_out, initial):
    steps, paths, width = increments.shape
    total = nd * width
    hid = w_in.shape[1]
    zscale = 2.0 / math.sqrt(total)
    d = lax.axis_index("dim")
    order = [m for m in range(nd) if m % 2 == 0] + [m for m in range(nd) if m % 2 == 1]
    half = nd // 2
    in_blocks = [lax.dynamic_slice_in_dim(w_in, (d ^ m) * width, width, 0) for m in order]
    out_blocks = [lax.dynamic_slice_in_dim(w_out, (d ^ m) * width, width, 1) for m in order]
    in_near, in_far = (jnp.concatenate(in_blocks[:half], 0), jnp.concatenate(in_blocks[half:], 0))
    out_near, out_far = (jnp.concatenate(out_blocks[:half], 1), jnp.concatenate(out_blocks[half:], 1))

    rows = paths // chunks
    n = steps * rows
    states, norms, incs = [], [], []
    for c in range(chunks):
        inc = increments[:, c * rows : (c + 1) * rows]
        state = start[c * rows : (c + 1) * rows]
        seen = []
        for step in range(steps):
            seen.append(state.astype(bf16))
            state = state + noise_coef * inc[step]
        states.append(jnp.concatenate(seen, 0))
        norms.append(jnp.sum(state * state, 1))
        incs.append(inc.reshape(n, width))

    xs, hs, acts, us, sums = [], [], [], [], []
    for c in range(chunks):
        xs.append(gather_cols(states[c], nd, c % 2 == 1))
    for c in range(chunks):
        near, far = xs[c]
        hidden = mm(near, in_near) + mm(far, in_far)
        hs.append(hidden)
        acts.append(jax.nn.silu(hidden).astype(bf16))
    for c in range(chunks):
        far = mm(acts[c], out_far).astype(bf16)
        zval = zscale * scatter_sum(mm(acts[c], out_near), far, nd, width, c % 2 == 1)
        inc = incs[c]
        us.append((zscale * (lam_coef * time_step * zval + inc)).astype(bf16))
        term = jnp.sum(0.5 * lam_coef * time_step * zval * zval + zval * inc, 1)
        sums.append(jnp.sum(term.reshape(steps, rows), 0))
    act_all = [gather_batch(a, nb) for a in acts]
    ug = [gather_cols(us[c], nd, c % 2 == 1) for c in range(chunks)]

    both = jnp.stack([jnp.concatenate(sums), jnp.concatenate(norms)])
    bit = 1
    while bit < nd:
        both = both + swap(both, "dim", nd, bit)
        bit *= 2
    residual = initial + both[0] - jnp.log((1.0 + both[1]) * 0.5)

    ghs, ucs, xcs = [], [], []
    for c in range(chunks):
        scale = jnp.tile(residual[c * rows : (c + 1) * rows], steps)[:, None]
        near, far = ug[c]
        ga = scale * (mm(near, out_near, 1, 1) + mm(far, out_far, 1, 1))
        sig = jax.nn.sigmoid(hs[c])
        ghs.append((ga * sig * (1.0 + hs[c] * (1.0 - sig))).astype(bf16))
        xcs.append(jnp.concatenate(column_share(*xs[c], nd, nb, width), 0))
        ucs.append(jnp.concatenate(column_share(near, far, nd, nb, width, scale), 0))
    gh_all = [gather_batch(g, nb) for g in ghs]

    def spread(parts):
        mid = len(parts) // 2
        first = gather_cols(jnp.concatenate(parts[:mid], 0), nd, False)
        second = gather_cols(jnp.concatenate(parts[mid:], 0), nd, True)
        return jnp.concatenate([jnp.concatenate(p, 1) for p in (first, second)], 0)

    share = total // nb // nd
    x_cols, u_cols = spread(xcs), spread(ucs)
    grad_in = mm(x_cols, jnp.concatenate(gh_all, 0), 0, 0)
    grad_out = mm(jnp.concatenate(act_all, 0), u_cols, 0, 0)
    where = [((e ^ d) & 1) * half + ((e ^ d) >> 1) for e in range(nd)]
    grad_in = jnp.concatenate([lax.dynamic_slice_in_dim(grad_in, w * share, share, 0) for w in where], 0)
    grad_out = jnp.concatenate([lax.dynamic_slice_in_dim(grad_out, w * share, share, 1) for w in where], 1)
    return (residual, grad_in, grad_out)


def solution(mesh):
    nd, nb = mesh.shape["dim"], mesh.shape["batch"]
    return jax.shard_map(
        functools.partial(on_device, nd, nb, 4),
        mesh=mesh,
        in_specs=(P("batch", "dim"), P(None, "batch", "dim"), P(None, "dim"), P("dim", None), P()),
        out_specs=(P("batch"), P("batch", "dim"), P("dim", "batch")),
        check_vma=False,
    )
```
